32 devices in a mesh: gx: 4 (over x, core), gy: 4 (over z), gz: 2 (over y).
Axes of the slice: x: 2, y: 2, z: 4, core: 2. Of those that a mesh axis runs over, the one named last changes fastest.
Arguments:
- orbitals: float32 [16, 48, 48, 256], P(None, 'gx', 'gy', 'gz'), may hold values from -6 to 6
- potential: float32 [48, 48, 256], P('gx', 'gy', 'gz'), may hold values from 0 to 2
Outputs:
- filtered: float32 [16, 48, 48, 256], P(None, 'gx', 'gy', 'gz')
The draws below stay inside these ranges and needn't reach their ends.
All inputs are finite; a program needn't handle non-finite values.
Results may differ from the reference program's by a relative error of at most 0.00002.
Values sent between devices are 32-bit elements; how exact they have to be, the bound alone decides.
A program may use at most 64 MiB of HBM per device.

```python
import jax
import jax.numpy as jnp
from jax import lax

BANDS = 16
DEGREE = 2
NX = 48
NY = 48
NZ = 256


def level_of(key, dims, cuts, least, high):
    loudness = 1.0
    for axis_at, blocks in cuts:
        heights = jax.random.uniform(jax.random.fold_in(jax.random.fold_in(key, 6), axis_at), (blocks,), jnp.float32, least / len(cuts), high / len(cuts))
        loudness = loudness * jnp.repeat(jnp.exp(heights), dims[axis_at] // blocks).reshape((-1,) + (1,) * (len(dims) - 1 - axis_at))
    return loudness


def normal_values(stream_key, dims, scale, most, split=(), kind=jnp.bfloat16):
    level = level_of(stream_key, dims, split, -0.22, 0.18) if split else 1.0
    array = jax.random.normal(stream_key, dims, jnp.float32) * scale * level
    return jnp.minimum(jnp.maximum(array, -most), most).astype(kind)


def setup_inputs(seed: int = 0) -> dict:
    streams_of = jax.random.split(jax.random.key(seed), 3)
    return {
        "orbitals": normal_values(streams_of[0], (BANDS, NX, NY, NZ), 1.0, 6.0, ((1, 4), (2, 4), (3, 2)), jnp.float32),
        "potential": jnp.clip(2.0 * jax.random.uniform(streams_of[1], (NX, NY, NZ), jnp.float32) ** level_of(streams_of[1], (NX, NY, NZ), ((0, 4), (1, 4), (2, 2)), -0.2, 0.2), 0.0, 2.0),
    }


SECOND = (-5369.0 / 1800.0, 12.0 / 7.0, -15.0 / 56.0, 10.0 / 189.0, -1.0 / 112.0, 2.0 / 1925.0, -1.0 / 16632.0)
FIRST = (6.0 / 7.0, -15.0 / 56.0, 5.0 / 63.0, -1.0 / 56.0, 3.0 / 385.0, -1.0 / 792.0)
METRIC = ((1.0, 0.25, 0.15), (0.25, 1.0, 0.2), (0.15, 0.2, 1.0))
CENTER = 10.5
HALF_WIDTH = 9.5


def window(values, starts, lengths):
    leading = values.ndim - 3
    starts_full = (0,) * leading + tuple(starts)
    limits = tuple(values.shape[:leading]) + tuple(s + l for s, l in zip(starts, lengths))
    return lax.slice(values, starts_full, limits)


def apply_operator(padded, potential):
    lengths = [padded.shape[i + 1] - 12 for i in range(3)]
    centre = window(padded, (6, 6, 6), lengths)
    summed = METRIC[0][0] * 0.0 * centre
    for d in range(3):
        second = SECOND[0] * centre
        for k in range(1, 7):
            forward = [6, 6, 6]
            forward[d] += k
            backward = [6, 6, 6]
            backward[d] -= k
            second = second + SECOND[k] * (window(padded, forward, lengths) + window(padded, backward, lengths))
        summed = summed + METRIC[d][d] * second
    for d, e in ((0, 1), (0, 2), (1, 2)):
        widened = list(lengths)
        widened[d] += 12
        partial_sum = None
        for k in range(1, 7):
            forward = [6, 6, 6]
            forward[d] = 0
            forward[e] += k
            backward = [6, 6, 6]
            backward[d] = 0
            backward[e] -= k
            term = FIRST[k - 1] * (window(padded, forward, widened) - window(padded, backward, widened))
            partial_sum = term if partial_sum is None else partial_sum + term
        crossed = None
        for k in range(1, 7):
            forward = [0, 0, 0]
            forward[d] = 6 + k
            backward = [0, 0, 0]
            backward[d] = 6 - k
            term = FIRST[k - 1] * (window(partial_sum, forward, lengths) - window(partial_sum, backward, lengths))
            crossed = term if crossed is None else crossed + term
        summed = summed + 2.0 * METRIC[d][e] * crossed
    return -0.5 * summed + potential[None] * centre


def reference(orbitals, potential):
    previous = jnp.zeros_like(orbitals)
    current = orbitals
    for degree_step in range(DEGREE):
        padded = jnp.pad(current, ((0, 0), (6, 6), (6, 6), (6, 6)), mode="wrap")
        applied = apply_operator(padded, potential)
        factor = 1.0 if degree_step == 0 else 2.0
        carry_factor = 0.0 if degree_step == 0 else 1.0
        following = factor * (applied - CENTER * current) / HALF_WIDTH - carry_factor * previous
        previous = current
        current = following
    return current
```

```python
import functools

import jax
import jax.numpy as jnp
import numpy as np
from jax import lax
from jax.experimental import pallas as pl
from jax.experimental.pallas import tpu as pltpu
from jax.sharding import PartitionSpec as P

DEGREE = 2
SECOND = (
    -5369.0 / 1800.0,
    12.0 / 7.0,
    -15.0 / 56.0,
    10.0 / 189.0,
    -1.0 / 112.0,
    2.0 / 1925.0,
    -1.0 / 16632.0,
)
FIRST = (6.0 / 7.0, -15.0 / 56.0, 5.0 / 63.0, -1.0 / 56.0, 3.0 / 385.0, -1.0 / 792.0)
METRIC = ((1.0, 0.25, 0.15), (0.25, 1.0, 0.2), (0.15, 0.2, 1.0))
CENTER = 10.5
HALF_WIDTH = 9.5
R = 6
Y0 = 8
MESH = pl.DeviceIdType.MESH


def z_matrices(bz):
    w = np.zeros((bz + 128, 2 * bz), np.float64)

    def row(p):
        return p if 0 <= p < bz else (bz + 8 + p if p < 0 else p + 8)

    for n in range(bz):
        for k in range(1, R + 1):
            w[row(n + k), n] += FIRST[k - 1]
            w[row(n - k), n] -= FIRST[k - 1]
            w[row(n + k), bz + n] += -0.5 * METRIC[2][2] * SECOND[k]
            w[row(n - k), bz + n] += -0.5 * METRIC[2][2] * SECOND[k]
    high = w.astype(np.float32).astype(jnp.bfloat16)
    low = (w - high.astype(np.float64)).astype(np.float32).astype(jnp.bfloat16)
    return jnp.asarray(high), jnp.asarray(low)


def kernel(
    gx, gy, gz,
    orb, pot, whi_ref, wlo_ref, out,
    vin, pin, v0, v1, a_ref, c_ref, s_ref, obuf, ebuf, hbuf,
    isend, irecv, psend, precv, qsend, qrecv, hsend, hrecv, osend, orecv, lsem,
):
    _, bx, by, bz = orb.shape
    nx, ny = gx * bx, gy * by
    cx, cy, cz = lax.axis_index("gx"), lax.axis_index("gy"), lax.axis_index("gz")
    band = cx * gy + cy
    zl, zr = lax.rem(cz + gz - 1, gz), lax.rem(cz + 1, gz)
    peers = [(dx, dy) for dx in range(gx) for dy in range(gy) if dx or dy]
    order = sorted(peers, key=lambda d: -min(d[1], gy - d[1]))

    def there(dx, dy):
        return lax.rem(cx + dx, gx), lax.rem(cy + dy, gy)

    barrier = pltpu.get_barrier_semaphore()
    for dx, dy in peers:
        tx, ty = there(dx, dy)
        pl.semaphore_signal(barrier, inc=1, device_id=(tx, ty, cz), device_id_type=MESH)
    for z in (zl, zr):
        pl.semaphore_signal(barrier, inc=1, device_id=(cx, cy, z), device_id_type=MESH)
    pl.semaphore_wait(barrier, len(peers) + 2)

    own = pltpu.make_async_copy(orb.at[band], vin.at[cx, cy], lsem.at[0])
    own.start()
    own_pot = pltpu.make_async_copy(pot, pin.at[cx, cy], lsem.at[1])
    own_pot.start()
    incoming = []
    for dx, dy in order:
        tx, ty = there(dx, dy)
        i = dx * gy + dy
        copy = pltpu.make_async_remote_copy(
            orb.at[tx * gy + ty], vin.at[cx, cy], isend.at[i], irecv.at[i],
            device_id=(tx, ty, cz), device_id_type=MESH,
        )
        copy.start()
        incoming.append(copy)
    gathers = []
    for dy in range(1, gy):
        copy = pltpu.make_async_remote_copy(
            pot, pin.at[cx, cy], psend.at[dy], precv.at[dy],
            device_id=(cx, lax.rem(cy + dy, gy), cz), device_id_type=MESH,
        )
        copy.start()
        gathers.append(copy)
    own.wait()
    for copy in incoming:
        copy.wait()

    def wrap_y(ref, x):
        ref[x, pl.ds(Y0 - R, R), :] = ref[x, pl.ds(Y0 + ny - R, R), :]
        ref[x, pl.ds(Y0 + ny, R), :] = ref[x, pl.ds(Y0, R), :]

    def wrap_x(ref):
        ref[pl.ds(0, R)] = ref[pl.ds(nx, R)]
        ref[pl.ds(nx + R, R)] = ref[pl.ds(R, R)]

    for sx in range(gx):
        @pl.loop(0, bx)
        def _(i):
            x = sx * bx + i + R
            for sy in range(gy):
                v0[x, pl.ds(Y0 + sy * by, by), :] = vin[sx, sy, i]
            wrap_y(v0, x)
    wrap_x(v0)

    xc = 8
    rows = xc * ny
    blocks = rows // 128

    def send_edges(step, v):
        @pl.loop(0, nx // xc)
        def _(c):
            vals = v[pl.ds(c * xc + R, xc), pl.ds(Y0, ny), :].reshape(rows, bz)
            for i in range(blocks):
                at = pl.multiple_of(c * rows + i * 128, 128)
                t = vals[i * 128 : (i + 1) * 128].T
                ebuf[step, 0, :, pl.ds(at, 128)] = t[:8]
                ebuf[step, 1, :, pl.ds(at, 128)] = t[bz - 8 :]

        copies = []
        for side, z in ((0, zl), (1, zr)):
            copy = pltpu.make_async_remote_copy(
                ebuf.at[step, side], hbuf.at[step, 1 - side],
                hsend.at[step, side], hrecv.at[step, 1 - side],
                device_id=(cx, cy, z), device_id_type=MESH,
            )
            copy.start()
            copies.append(copy)
        return copies

    def y_pass(v):
        @pl.loop(0, nx)
        def _(x):
            first = second = None
            for k in range(1, R + 1):
                up = v[x + R, pl.ds(Y0 + k, ny), :]
                down = v[x + R, pl.ds(Y0 - k, ny), :]
                f = (-METRIC[0][1] * FIRST[k - 1]) * (up - down)
                s = (-0.5 * METRIC[1][1] * SECOND[k]) * (up + down)
                first = f if first is None else first + f
                second = s if second is None else second + s
            c_ref[x + R] = first
            s_ref[x] = second

    def z_pass(step, v):
        @pl.loop(0, nx // xc)
        def _(c):
            vals = v[pl.ds(c * xc + R, xc), pl.ds(Y0, ny), :].reshape(rows, bz)
            sides = []
            for i in range(blocks):
                at = pl.multiple_of(c * rows + i * 128, 128)
                block = jnp.concatenate(
                    [
                        hbuf[step, 0, :, pl.ds(at, 128)],
                        hbuf[step, 1, :, pl.ds(at, 128)],
                        jnp.zeros((112, 128), jnp.float32),
                    ],
                    axis=0,
                )
                sides.append(block.T)
            full = jnp.concatenate([vals, jnp.concatenate(sides, axis=0)], axis=1)
            high = full.astype(jnp.bfloat16)
            low = (full - high.astype(jnp.float32)).astype(jnp.bfloat16)
            dot = functools.partial(jnp.dot, preferred_element_type=jnp.float32)
            whi = whi_ref[...]
            got = dot(high, whi) + (dot(low, whi) + dot(high, wlo_ref[...]))
            a = got[:, :bz].reshape(xc, ny, bz)
            s_ref[pl.ds(c * xc, xc)] += got[:, bz:].reshape(xc, ny, bz)
            c_ref[pl.ds(c * xc + R, xc)] += (-METRIC[0][2]) * a
            a_ref[pl.ds(c * xc, xc), pl.ds(Y0, ny), :] = a
            for i in range(xc):
                wrap_y(a_ref, c * xc + i)

        wrap_x(c_ref)

    def x_row(v, x, sx, i):
        centre = v[x + R, pl.ds(Y0, ny), :]
        local_pot = jnp.concatenate([pin[sx, sy, i] for sy in range(gy)], axis=0)
        total = s_ref[x] + (local_pot + (-1.5 * SECOND[0] - CENTER)) * centre
        for k in range(1, R + 1):
            total = total + (-0.5 * METRIC[0][0] * SECOND[k]) * (
                v[x + R + k, pl.ds(Y0, ny), :] + v[x + R - k, pl.ds(Y0, ny), :]
            )
            total = total + FIRST[k - 1] * (c_ref[x + R + k] - c_ref[x + R - k])
            total = total + (-METRIC[1][2] * FIRST[k - 1]) * (
                a_ref[x, pl.ds(Y0 + k, ny), :] - a_ref[x, pl.ds(Y0 - k, ny), :]
            )
        return total

    edges = send_edges(0, v0)
    y_pass(v0)
    own_pot.wait()
    for copy in gathers:
        copy.wait()
    spread = []
    for dx in range(1, gx):
        copy = pltpu.make_async_remote_copy(
            pin.at[cx], pin.at[cx], qsend.at[dx], qrecv.at[dx],
            device_id=(lax.rem(cx + dx, gx), cy, cz), device_id_type=MESH,
        )
        copy.start()
        spread.append(copy)
    for copy in edges:
        copy.wait()
    z_pass(0, v0)
    for copy in spread:
        copy.wait()
    for sx in range(gx):
        @pl.loop(0, bx)
        def _(i):
            x = sx * bx + i
            v1[x + R, pl.ds(Y0, ny), :] = (1.0 / HALF_WIDTH) * x_row(v0, x, sx, i)
            wrap_y(v1, x + R)
    wrap_x(v1)

    edges = send_edges(1, v1)
    y_pass(v1)
    for copy in edges:
        copy.wait()
    z_pass(1, v1)
    outgoing = []
    for dx in list(range(1, gx)) + [0]:
        tx = lax.rem(cx + dx, gx)

        @pl.loop(0, bx)
        def _(i):
            x = tx * bx + i
            got = (2.0 / HALF_WIDTH) * x_row(v1, x, tx, i) - v0[x + R, pl.ds(Y0, ny), :]
            for sy in range(gy):
                obuf[tx, sy, i] = got[sy * by : (sy + 1) * by]

        for dy in sorted(range(gy), key=lambda d: -min(d, gy - d)):
            ty = lax.rem(cy + dy, gy)
            n = dx * gy + dy
            if n == 0:
                copy = pltpu.make_async_copy(obuf.at[tx, ty], out.at[band], lsem.at[2])
            else:
                copy = pltpu.make_async_remote_copy(
                    obuf.at[tx, ty], out.at[band], osend.at[n], orecv.at[n],
                    device_id=(tx, ty, cz), device_id_type=MESH,
                )
            copy.start()
            outgoing.append(copy)
    for copy in outgoing:
        copy.wait()


def local(sizes, orbitals, potential):
    gx, gy, gz = sizes
    bands, bx, by, bz = orbitals.shape
    nx, ny = gx * bx, gy * by
    assert bands == gx * gy and gz > 1
    f32 = jnp.float32
    whi, wlo = z_matrices(bz)
    anywhere = pl.BlockSpec(memory_space=pl.ANY)
    vmem = pl.BlockSpec(memory_space=pltpu.VMEM)
    dma = pltpu.SemaphoreType.DMA
    return pl.pallas_call(
        functools.partial(kernel, gx, gy, gz),
        out_shape=jax.ShapeDtypeStruct(orbitals.shape, f32),
        in_specs=[anywhere, anywhere, vmem, vmem],
        out_specs=anywhere,
        scratch_shapes=[
            pltpu.VMEM((gx, gy, bx, by, bz), f32),
            pltpu.VMEM((gx, gy, bx, by, bz), f32),
            pltpu.VMEM((nx + 2 * R, ny + 16, bz), f32),
            pltpu.VMEM((nx + 2 * R, ny + 16, bz), f32),
            pltpu.VMEM((nx, ny + 16, bz), f32),
            pltpu.VMEM((nx + 2 * R, ny, bz), f32),
            pltpu.VMEM((nx, ny, bz), f32),
            pltpu.VMEM((gx, gy, bx, by, bz), f32),
            pltpu.VMEM((DEGREE, 2, 8, nx * ny), f32),
            pltpu.VMEM((DEGREE, 2, 8, nx * ny), f32),
            dma((gx * gy,)), dma((gx * gy,)),
            dma((gy,)), dma((gy,)),
            dma((gx,)), dma((gx,)),
            dma((DEGREE, 2)), dma((DEGREE, 2)),
            dma((gx * gy,)), dma((gx * gy,)),
            dma((3,)),
        ],
        compiler_params=pltpu.CompilerParams(
            collective_id=0, has_side_effects=True, vmem_limit_bytes=48 * 1024 * 1024
        ),
    )(orbitals, potential, whi, wlo)


def solution(mesh):
    sizes = tuple(mesh.shape[a] for a in ("gx", "gy", "gz"))
    return jax.shard_map(
        functools.partial(local, sizes),
        mesh=mesh,
        in_specs=(P(None, "gx", "gy", "gz"), P("gx", "gy", "gz")),
        out_specs=P(None, "gx", "gy", "gz"),
        check_vma=False,
    )
```

```python
import functools
import math

import jax
import jax.numpy as jnp
import numpy as np
from jax import lax
from jax.experimental import pallas as pl
from jax.experimental.pallas import tpu as pltpu
from jax.sharding import PartitionSpec as P

DEGREE = 2
SECOND = (
    -5369.0 / 1800.0,
    12.0 / 7.0,
    -15.0 / 56.0,
    10.0 / 189.0,
    -1.0 / 112.0,
    2.0 / 1925.0,
    -1.0 / 16632.0,
)
FIRST = (6.0 / 7.0, -15.0 / 56.0, 5.0 / 63.0, -1.0 / 56.0, 3.0 / 385.0, -1.0 / 792.0)
METRIC = ((1.0, 0.25, 0.15), (0.25, 1.0, 0.2), (0.15, 0.2, 1.0))
CENTER = 10.5
HALF_WIDTH = 9.5
R = 6
Y0 = 8
MESH = pl.DeviceIdType.MESH


def z_matrices(bz):
    w = np.zeros((bz + 128, 2 * bz), np.float64)

    def row(p):
        return p if 0 <= p < bz else (bz + 8 + p if p < 0 else p + 8)

    for n in range(bz):
        for k in range(1, R + 1):
            w[row(n + k), n] += FIRST[k - 1]
            w[row(n - k), n] -= FIRST[k - 1]
            w[row(n + k), bz + n] += -0.5 * METRIC[2][2] * SECOND[k]
            w[row(n - k), bz + n] += -0.5 * METRIC[2][2] * SECOND[k]
    high = w.astype(np.float32).astype(jnp.bfloat16)
    low = (w - high.astype(np.float64)).astype(np.float32).astype(jnp.bfloat16)
    return jnp.asarray(high), jnp.asarray(low)


def kernel(
    gx, gy, gz, bx, by,
    orb, pot, whi_ref, wlo_ref, out,
    vin, pin, p_ref, v0, v1, a_ref, c0, c1, s_ref, obuf, ebuf, hbuf,
    isend, irecv, psend, precv, qsend, qrecv, hsend, hrecv, osend, orecv, lsem,
):
    bz = orb.shape[-1]
    nx, ny = gx * bx, gy * by
    group = 8 // math.gcd(by, 8)
    rows = bx * ny
    padded_rows = ebuf.shape[-1]
    cx, cy, cz = lax.axis_index("gx"), lax.axis_index("gy"), lax.axis_index("gz")
    band = cx * gy + cy
    zl, zr = lax.rem(cz + gz - 1, gz), lax.rem(cz + 1, gz)
    far_first = sorted(range(1, gy), key=lambda d: -min(d, gy - d))

    barrier = pltpu.get_barrier_semaphore()
    for dx in range(gx):
        for dy in range(gy):
            if dx or dy:
                pl.semaphore_signal(
                    barrier, inc=1,
                    device_id=(lax.rem(cx + dx, gx), lax.rem(cy + dy, gy), cz),
                    device_id_type=MESH,
                )
    for z in (zl, zr):
        pl.semaphore_signal(barrier, inc=1, device_id=(cx, cy, z), device_id_type=MESH)
    pl.semaphore_wait(barrier, gx * gy + 1)

    own_pot = pltpu.make_async_copy(pot, pin.at[cx, cy], lsem.at[1])
    own_pot.start()
    gathers = [own_pot]
    for dy in far_first:
        copy = pltpu.make_async_remote_copy(
            pot, pin.at[cx, cy], psend.at[dy], precv.at[dy],
            device_id=(cx, lax.rem(cy + dy, gy), cz), device_id_type=MESH,
        )
        copy.start()
        gathers.append(copy)

    def send_bands(dx):
        tx = lax.rem(cx + dx, gx)
        copies = []
        for dy in far_first + [0]:
            ty = lax.rem(cy + dy, gy)
            n = dx * gy + dy
            if n == 0:
                copy = pltpu.make_async_copy(orb.at[band], vin.at[cx, cy], lsem.at[0])
            else:
                copy = pltpu.make_async_remote_copy(
                    orb.at[tx * gy + ty], vin.at[cx, cy], isend.at[n], irecv.at[n],
                    device_id=(tx, ty, cz), device_id_type=MESH,
                )
            copy.start()
            copies.append(copy)
        return copies

    spread_steps = []
    d = gx // 2
    while d:
        spread_steps.append(d)
        d //= 2
    held = [cx]
    spread_count = [0]

    def spread(d):
        bit = lax.rem(lax.div(cx, d), 2)
        hop = d - 2 * d * bit
        copies = []
        for r in list(held):
            i = spread_count[0]
            spread_count[0] += 1
            copy = pltpu.make_async_remote_copy(
                pin.at[r], pin.at[r], qsend.at[i], qrecv.at[i],
                device_id=(cx + hop, cy, cz), device_id_type=MESH,
            )
            copy.start()
            copies.append(copy)
            held.append(r + hop)
        return copies

    def wrap_y(ref, x):
        ref[x, pl.ds(Y0 - R, R), :] = ref[x, pl.ds(Y0 + ny - R, R), :]
        ref[x, pl.ds(Y0 + ny, R), :] = ref[x, pl.ds(Y0, R), :]

    def wrap_x(ref, sx):
        @pl.when(sx == 0)
        def _():
            ref[pl.ds(nx + R, R)] = ref[pl.ds(R, R)]

        @pl.when(sx == gx - 1)
        def _():
            ref[pl.ds(0, R)] = ref[pl.ds(nx, R)]

    def pieces(ref, sx, i):
        at = pl.multiple_of(i * group * by, 8)
        for sy in range(gy):
            got = ref[sx, sy, pl.ds(at, group * by), :]
            for j in range(group):
                yield sy, j, got[j * by : (j + 1) * by]

    def assemble(sx):
        @pl.loop(0, bx // group)
        def _(i):
            x = sx * bx + i * group + R
            for sy, j, piece in pieces(vin, sx, i):
                v0[x + j, pl.ds(Y0 + sy * by, by), :] = piece
            for j in range(group):
                wrap_y(v0, x + j)
        wrap_x(v0, sx)

    def assemble_potential():
        for sx in range(gx):
            @pl.loop(0, bx // group)
            def _(i):
                x = sx * bx + i * group
                for sy, j, piece in pieces(pin, sx, i):
                    p_ref[x + j, pl.ds(sy * by, by), :] = piece + (-1.5 * SECOND[0] - CENTER)

    def send_edges(step, v, sx, t):
        vals = v[pl.ds(sx * bx + R, bx), pl.ds(Y0, ny), :].reshape(rows, bz)
        if padded_rows > rows:
            vals = jnp.concatenate([vals, jnp.zeros((padded_rows - rows, bz), jnp.float32)], axis=0)
        for i in range(padded_rows // 128):
            turned = vals[i * 128 : (i + 1) * 128].T
            ebuf[step, t, 0, :, pl.ds(i * 128, 128)] = turned[:8]
            ebuf[step, t, 1, :, pl.ds(i * 128, 128)] = turned[bz - 8 :]
        copies = []
        for side, z in ((0, zl), (1, zr)):
            copy = pltpu.make_async_remote_copy(
                ebuf.at[step, t, side], hbuf.at[step, t, 1 - side],
                hsend.at[step, t, side], hrecv.at[step, t, 1 - side],
                device_id=(cx, cy, z), device_id_type=MESH,
            )
            copy.start()
            copies.append(copy)
        return copies

    def y_pass(v, c_ref, sx):
        @pl.loop(0, bx)
        def _(i):
            x = sx * bx + i
            first = second = None
            for k in range(1, R + 1):
                up = v[x + R, pl.ds(Y0 + k, ny), :]
                down = v[x + R, pl.ds(Y0 - k, ny), :]
                f = (-METRIC[0][1] * FIRST[k - 1]) * (up - down)
                s = (-0.5 * METRIC[1][1] * SECOND[k]) * (up + down)
                first = f if first is None else first + f
                second = s if second is None else second + s
            c_ref[x + R] = first
            s_ref[x] = second

    def z_pass(step, v, c_ref, sx, t):
        vals = v[pl.ds(sx * bx + R, bx), pl.ds(Y0, ny), :].reshape(rows, bz)
        sides = []
        for i in range(padded_rows // 128):
            block = jnp.concatenate(
                [
                    hbuf[step, t, 0, :, pl.ds(i * 128, 128)],
                    hbuf[step, t, 1, :, pl.ds(i * 128, 128)],
                    jnp.zeros((112, 128), jnp.float32),
                ],
                axis=0,
            )
            sides.append(block.T)
        full = jnp.concatenate([vals, jnp.concatenate(sides, axis=0)[:rows]], axis=1)
        high = full.astype(jnp.bfloat16)
        low = (full - high.astype(jnp.float32)).astype(jnp.bfloat16)
        dot = functools.partial(jnp.dot, preferred_element_type=jnp.float32)
        whi = whi_ref[...]
        got = dot(high, whi) + (dot(low, whi) + dot(high, wlo_ref[...]))
        a = got[:, :bz].reshape(bx, ny, bz)
        s_ref[pl.ds(sx * bx, bx)] += got[:, bz:].reshape(bx, ny, bz)
        c_ref[pl.ds(sx * bx + R, bx)] += (-METRIC[0][2]) * a
        a_ref[pl.ds(sx * bx, bx), pl.ds(Y0, ny), :] = a
        for i in range(bx):
            wrap_y(a_ref, sx * bx + i)
        wrap_x(c_ref, sx)

    def x_row(v, c_ref, x):
        total = s_ref[x] + p_ref[x] * v[x + R, pl.ds(Y0, ny), :]
        for k in range(1, R + 1):
            total = total + (-0.5 * METRIC[0][0] * SECOND[k]) * (
                v[x + R + k, pl.ds(Y0, ny), :] + v[x + R - k, pl.ds(Y0, ny), :]
            )
            total = total + FIRST[k - 1] * (c_ref[x + R + k] - c_ref[x + R - k])
            total = total + (-METRIC[1][2] * FIRST[k - 1]) * (
                a_ref[x, pl.ds(Y0 + k, ny), :] - a_ref[x, pl.ds(Y0 - k, ny), :]
            )
        return total

    def wait_all(copies):
        for copy in copies:
            copy.wait()

    block = [lax.rem(cx + gx - t, gx) for t in range(gx)]
    second_edges = {}

    def first_x_pass(t):
        sx = block[t]

        @pl.loop(0, bx)
        def _(i):
            x = sx * bx + i
            v1[x + R, pl.ds(Y0, ny), :] = (1.0 / HALF_WIDTH) * x_row(v0, c0, x)
            wrap_y(v1, x + R)
        wrap_x(v1, sx)
        second_edges[t] = send_edges(1, v1, sx, t)
        y_pass(v1, c1, sx)

    half = (gx + 1) // 2
    bands_in = [send_bands(dx) for dx in range(half)]
    wait_all(gathers)
    doing = spread(spread_steps[0])
    bands_in += [send_bands(dx) for dx in range(half, gx)]
    first_edges = []
    for t in range(gx):
        wait_all(bands_in[t])
        assemble(block[t])
        first_edges.append(send_edges(0, v0, block[t], t))
        y_pass(v0, c0, block[t])
        if 1 <= t < gx - 1:
            wait_all(doing)
            doing = spread(spread_steps[t]) if t < len(spread_steps) else []
        if t == gx - 1:
            wait_all(doing)
            assemble_potential()
        if t >= 1:
            wait_all(first_edges[t - 1])
            z_pass(0, v0, c0, block[t - 1], t - 1)
    for t in range(1, gx - 2):
        first_x_pass(t)
    wait_all(first_edges[gx - 1])
    z_pass(0, v0, c0, block[gx - 1], gx - 1)
    late = [gx - 2, gx - 1, 0]
    for t in late:
        first_x_pass(t)

    outgoing = []

    def last_x_pass(t):
        sx = block[t]

        @pl.loop(0, bx // group)
        def _(i):
            got = []
            for j in range(group):
                x = sx * bx + i * group + j
                got.append(
                    (2.0 / HALF_WIDTH) * x_row(v1, c1, x) - v0[x + R, pl.ds(Y0, ny), :]
                )
            at = pl.multiple_of(i * group * by, 8)
            for sy in range(gy):
                obuf[sx, sy, pl.ds(at, group * by), :] = jnp.concatenate(
                    [g[sy * by : (sy + 1) * by] for g in got], axis=0
                )

        for dy in far_first + [0]:
            ty = lax.rem(cy + dy, gy)
            n = t * gy + dy
            if n == 0:
                copy = pltpu.make_async_copy(obuf.at[sx, ty], out.at[band], lsem.at[2])
            else:
                copy = pltpu.make_async_remote_copy(
                    obuf.at[sx, ty], out.at[band], osend.at[n], orecv.at[n],
                    device_id=(sx, ty, cz), device_id_type=MESH,
                )
            copy.start()
            outgoing.append(copy)

    ready = list(range(1, gx - 2)) + late
    done = []
    for t in ready:
        wait_all(second_edges[t])
        z_pass(1, v1, c1, block[t], t)
        done.append(t)
        for u in range(gx):
            near = {u, (u + 1) % gx, (u - 1) % gx}
            if near <= set(done) and t in near:
                last_x_pass(u)
    wait_all(outgoing)


def local(sizes, orbitals, potential):
    gx, gy, gz = sizes
    bands, bx, by, bz = orbitals.shape
    nx, ny = gx * bx, gy * by
    assert bands == gx * gy and gz > 1 and gx >= 4 and gx & (gx - 1) == 0
    f32 = jnp.float32
    whi, wlo = z_matrices(bz)
    anywhere = pl.BlockSpec(memory_space=pl.ANY)
    vmem = pl.BlockSpec(memory_space=pltpu.VMEM)
    dma = pltpu.SemaphoreType.DMA
    edge = (DEGREE, gx, 2, 8, (bx * ny + 127) // 128 * 128)
    out = pl.pallas_call(
        functools.partial(kernel, gx, gy, gz, bx, by),
        out_shape=jax.ShapeDtypeStruct((bands, bx * by, bz), f32),
        in_specs=[anywhere, anywhere, vmem, vmem],
        out_specs=anywhere,
        scratch_shapes=[
            pltpu.VMEM((gx, gy, bx * by, bz), f32),
            pltpu.VMEM((gx, gy, bx * by, bz), f32),
            pltpu.VMEM((nx, ny, bz), f32),
            pltpu.VMEM((nx + 2 * R, ny + 16, bz), f32),
            pltpu.VMEM((nx + 2 * R, ny + 16, bz), f32),
            pltpu.VMEM((nx, ny + 16, bz), f32),
            pltpu.VMEM((nx + 2 * R, ny, bz), f32),
            pltpu.VMEM((nx + 2 * R, ny, bz), f32),
            pltpu.VMEM((nx, ny, bz), f32),
            pltpu.VMEM((gx, gy, bx * by, bz), f32),
            pltpu.VMEM(edge, f32),
            pltpu.VMEM(edge, f32),
            dma((gx * gy,)), dma((gx * gy,)),
            dma((gy,)), dma((gy,)),
            dma((gx,)), dma((gx,)),
            dma((DEGREE, gx, 2)), dma((DEGREE, gx, 2)),
            dma((gx * gy,)), dma((gx * gy,)),
            dma((3,)),
        ],
        compiler_params=pltpu.CompilerParams(
            collective_id=0, has_side_effects=True, vmem_limit_bytes=48 * 1024 * 1024
        ),
    )(
        orbitals.reshape(bands, bx * by, bz),
        potential.reshape(bx * by, bz),
        whi,
        wlo,
    )
    return out.reshape(bands, bx, by, bz)


def solution(mesh):
    sizes = tuple(mesh.shape[a] for a in ("gx", "gy", "gz"))
    return jax.shard_map(
        functools.partial(local, sizes),
        mesh=mesh,
        in_specs=(P(None, "gx", "gy", "gz"), P("gx", "gy", "gz")),
        out_specs=P(None, "gx", "gy", "gz"),
        check_vma=False,
    )
```
